32 devices in a mesh: dom: 32 (over z, y, x, core).
Axes of the slice: x: 2, y: 2, z: 4, core: 2. Of those that a mesh axis runs over, the one named last changes fastest.
Arguments:
- features: bfloat16 [32768, 512], P('dom'), may hold values from -6 to 6
- embeddings: bfloat16 [32768, 128], P('dom'), may hold values from -6 to 6
- tile_values: bfloat16 [256, 4, 128, 128], P('dom'), may hold values from -4 to 4
- tile_columns: int32 [256, 4], P('dom'), may hold values from 0 to 11
- send_blocks: int32 [32, 2, 2], P('dom'), may hold values from 0 to 7
- send_count: int32 [32, 2], P('dom'), may hold values from 1 to 2, as said below
- hub_rows: int32 [64], P('dom'), may hold values from 0 to 1023, as said below
- hub_weight: bfloat16 [32768, 64], P('dom'), may hold values from -4 to 4
- degree: int32 [32768], P('dom'), may hold values from 16 to 64
Outputs:
- hop_features: bfloat16 [3, 32768, 512], P(None, 'dom')
- hop_embeddings: bfloat16 [3, 32768, 128], P(None, 'dom')
The draws below stay inside these ranges and needn't reach their ends.
Inputs may be any that keep to these rules, and one draw needn't show every extreme that they name: `send_count`: some partition sends 2 blocks to its right and some to its left. `hub_rows`: the 2 hub rows of each partition are distinct local row numbers.
All inputs are finite; a program needn't handle non-finite values.
Results may differ from the reference program's by a relative error of at most 0.012.
Values may be sent and summed in bfloat16 or wider, within the bound.
A program may use at most 64 MiB of HBM per device.

```python
import jax
import jax.numpy as jnp
from jax import lax

F = 512
E = 128
TILE = 128
ROWS_DEV = 1024
K = 4
SEND_MOST = 2
HUB_DEV = 2
HOPS = 3
ROWS = 32768
BLOCKS = 256
HUBS = 64
N_DOM = 32


def draw_send_count(key, part):
    counts = jax.random.randint(key, (N_DOM, 2), 1, SEND_MOST + 1)
    counts = counts.at[0, 1].set(SEND_MOST)
    counts = counts.at[N_DOM - 1, 0].set(SEND_MOST)
    return counts.astype(jnp.int32)


def draw_hub_rows(key, part):

    def one_device(device_index):
        return jax.random.permutation(jax.random.fold_in(key, device_index), ROWS_DEV)[:HUB_DEV]
    chosen = jax.vmap(one_device)(jnp.arange(N_DOM, dtype=jnp.int32))
    return chosen.reshape(-1).astype(jnp.int32)


def plant(array, stream_key, least, high):
    spot = [jax.random.randint(jax.random.fold_in(stream_key, axis), (), 0, length) for axis, length in enumerate(array.shape)]
    longest = array.shape.index(max(array.shape))
    next_to = spot[:longest] + [(spot[longest] + 1) % array.shape[longest]] + spot[longest + 1:]
    return array.at[tuple(spot)].set(least).at[tuple(next_to)].set(high)


def block_scale(own_key, shape, cuts, low, top_value):
    def one(dim, blocks):
        steps = jax.random.uniform(jax.random.fold_in(jax.random.fold_in(own_key, 6), dim), (blocks,), jnp.float32, low / len(cuts), top_value / len(cuts))
        return jnp.repeat(jnp.exp(steps), shape[dim] // blocks).reshape((-1,) + (1,) * (len(shape) - dim - 1))

    level = one(*cuts[0])
    for cut in cuts[1:]:
        level = level * one(*cut)
    return level


def scatter_about(rng, dims, spread, reach, pieces=(), kind=jnp.bfloat16):
    values = spread * jax.random.normal(rng, dims, jnp.float32)
    if pieces:
        values = values * block_scale(rng, dims, pieces, -0.22, 0.18)
    return jnp.clip(values, -reach, reach).astype(kind)


def setup_inputs(seed: int = 0) -> dict:
    key_of = jax.random.split(jax.random.key(seed), 10)
    features = scatter_about(key_of[0], (ROWS, F), 1.0, 6.0, ((0, 32),))
    embeddings = scatter_about(key_of[1], (ROWS, E), 1.0, 6.0, ((0, 32),))
    tile_values = scatter_about(key_of[2], (BLOCKS, K, TILE, TILE), 1.0, 4.0, ((0, 32),))
    tile_columns = plant(jax.random.randint(key_of[3], (BLOCKS, K), 0, ROWS_DEV // TILE + 2 * SEND_MOST), jax.random.fold_in(key_of[3], 1), 0, (ROWS_DEV // TILE + 2 * SEND_MOST) - 1).astype(jnp.int32)
    send_blocks = plant(jax.random.randint(key_of[4], (N_DOM, 2, SEND_MOST), 0, ROWS_DEV // TILE), jax.random.fold_in(key_of[4], 1), 0, (ROWS_DEV // TILE) - 1).astype(jnp.int32)
    send_count = draw_send_count(jax.random.fold_in(key_of[9], 71), 0)
    hub_rows = draw_hub_rows(jax.random.fold_in(key_of[9], 71), 0)
    hub_weight = scatter_about(key_of[7], (ROWS, HUBS), 1.0, 4.0, ((0, 32),))
    degree = plant(jax.random.randint(key_of[8], (ROWS,), 16, 65), jax.random.fold_in(key_of[8], 1), 16, 64).astype(jnp.int32)
    return {"features": features, "embeddings": embeddings, "tile_values": tile_values, "tile_columns": tile_columns, "send_blocks": send_blocks, "send_count": send_count, "hub_rows": hub_rows, "hub_weight": hub_weight, "degree": degree}


def reference(features, embeddings, tile_values, tile_columns, send_blocks, send_count, hub_rows, hub_weight, degree):
    feature_width = F + E
    block_count = ROWS_DEV // TILE
    device_count = N_DOM
    inverse_root = lax.rsqrt(degree.astype(jnp.float32)).reshape(device_count, ROWS_DEV, 1)
    current = jnp.concatenate([features, embeddings], axis=1).reshape(device_count, ROWS_DEV, feature_width)
    tiles_split = tile_values.reshape(device_count, block_count, K, TILE, TILE)
    columns_split = tile_columns.reshape(device_count, block_count, K).astype(jnp.int32)
    hubs_split = hub_rows.reshape(device_count, HUB_DEV).astype(jnp.int32)
    weight_split = hub_weight.reshape(device_count, ROWS_DEV, HUBS)
    live_slots = jnp.arange(SEND_MOST, dtype=jnp.int32)[None, None, :] < send_count[:, :, None]
    empty_rim = jnp.zeros((1, SEND_MOST, TILE, feature_width), jnp.bfloat16)
    results = []
    for hop_index in range(HOPS):
        scaled = (current.astype(jnp.float32) * inverse_root).astype(jnp.bfloat16)
        blocked = scaled.reshape(device_count, block_count, TILE, feature_width)
        outgoing = jax.vmap(lambda source, listed: source[listed])(blocked, send_blocks.astype(jnp.int32))
        outgoing = jnp.where(live_slots[:, :, :, None, None], outgoing, jnp.zeros_like(outgoing))
        from_left = jnp.concatenate([empty_rim, outgoing[:-1, 1]], axis=0)
        from_right = jnp.concatenate([outgoing[1:, 0], empty_rim], axis=0)
        extended = jnp.concatenate([blocked, from_left, from_right], axis=1)
        gathered_hubs = jax.vmap(lambda source, listed: source[listed])(scaled, hubs_split).reshape(HUBS, feature_width)

        def one_device(operands):
            buffer, tiles_here, columns_here, weight_here = operands
            picked = buffer[columns_here]
            local_part = jnp.einsum('bkij,bkjw->biw', tiles_here.astype(jnp.float32), picked.astype(jnp.float32))
            local_part = local_part.reshape(ROWS_DEV, feature_width)
            return local_part + jnp.dot(weight_here, gathered_hubs, preferred_element_type=jnp.float32)
        summed = lax.map(one_device, (extended, tiles_split, columns_split, weight_split))
        current = (summed * inverse_root).astype(jnp.bfloat16)
        results.append(current.reshape(ROWS, feature_width))
    stacked = jnp.stack(results)
    return (stacked[:, :, :F], stacked[:, :, F:])
```

```python
import functools

import jax
import jax.numpy as jnp
from jax import lax
from jax.experimental import pallas as pl
from jax.experimental.pallas import tpu as pltpu
from jax.sharding import PartitionSpec as P

HOPS = 3
LANES = 128
MESH = pl.DeviceIdType.MESH


def kernel(
    n, sizes, cols_ref, listed_ref, count_ref, hubs_ref,
    features, embeddings, tiles, weight, degree,
    out_f, out_e, *scratch,
):
    blocks, tile, taps, send_most, hub_dev, chunks, f_chunks = sizes
    per = tile // 16
    pairs = HOPS * chunks
    scratch = list(scratch)
    take = lambda count: [scratch.pop(0) for _ in range(count)]
    locals_, groups, exts, sends, hub_sends, hub_bufs = (take(pairs) for _ in range(6))
    inv, rim_send_sem, rim_recv_sem, hub_send_sem, hub_recv_sem = scratch
    me = lax.axis_index("dom")

    barrier = pltpu.get_barrier_semaphore()

    def greet(step, carry):
        pl.semaphore_signal(
            barrier, inc=1, device_id=(lax.rem(me + step, n),), device_id_type=MESH
        )
        return carry

    lax.fori_loop(1, n, greet, 0)

    roots = lax.rsqrt(degree[...].astype(jnp.float32)).T
    for b in range(blocks):
        inv[b] = jnp.broadcast_to(roots[:, b : b + 1], (tile, LANES))

    rim_zero = jnp.zeros((send_most, tile, LANES), jnp.bfloat16)

    @pl.when(me == 0)
    def _():
        for i in range(pairs):
            exts[i][blocks : blocks + send_most] = rim_zero

    @pl.when(me == n - 1)
    def _():
        for i in range(pairs):
            exts[i][blocks + send_most :] = rim_zero

    def rim_copy(i, side):
        first = blocks if side == 1 else blocks + send_most
        to = me + 1 if side == 1 else me - 1
        return pltpu.make_async_remote_copy(
            src_ref=sends[i].at[side],
            dst_ref=exts[i].at[pl.ds(first, send_most)],
            send_sem=rim_send_sem.at[i, side],
            recv_sem=rim_recv_sem.at[i, side],
            device_id=(to,),
            device_id_type=MESH,
        )

    def send(i):
        source = locals_[i]
        picked = []
        for q in range(hub_dev):
            row = hubs_ref[q]
            near = groups[i][lax.div(row, 16)].astype(jnp.float32)
            here = lax.broadcasted_iota(jnp.int32, near.shape, 0) == lax.rem(row, 16)
            picked.append(jnp.sum(jnp.where(here, near, 0.0), axis=0, keepdims=True))
        packed = jnp.concatenate(picked, axis=0).astype(jnp.bfloat16)
        hub_sends[i][...] = packed
        hub_bufs[i][me] = packed

        def spread(step, carry):
            pltpu.make_async_remote_copy(
                src_ref=hub_sends[i],
                dst_ref=hub_bufs[i].at[me],
                send_sem=hub_send_sem.at[i],
                recv_sem=hub_recv_sem.at[i],
                device_id=(lax.rem(me + step, n),),
                device_id_type=MESH,
            ).start()
            return carry

        lax.fori_loop(1, n, spread, 0)
        for side in range(2):
            for s in range(send_most):
                block = source[listed_ref[0, side, s]]
                keep = jnp.where(s < count_ref[0, side], 1.0, 0.0).astype(jnp.float32)
                sends[i][side, s] = (block.astype(jnp.float32) * keep).astype(jnp.bfloat16)

        @pl.when(me < n - 1)
        def _():
            rim_copy(i, 1).start()

        @pl.when(me > 0)
        def _():
            rim_copy(i, 0).start()

    def prepare(c):
        def one(b, carry):
            rows = pl.ds(pl.multiple_of(b * tile, tile), tile)
            if c < f_chunks:
                x = features[rows, c * LANES : (c + 1) * LANES]
            else:
                x = embeddings[rows, (c - f_chunks) * LANES : (c - f_chunks + 1) * LANES]
            z = (x.astype(jnp.float32) * inv[b]).astype(jnp.bfloat16)
            locals_[c][b] = z
            groups[c][pl.ds(b * per, per)] = z.reshape(per, 16, LANES)
            exts[c][b] = z
            return carry

        lax.fori_loop(0, blocks, one, 0)

    prepare(0)
    pl.semaphore_wait(barrier, n - 1)
    send(0)
    for c in range(1, chunks):
        prepare(c)
        send(c)

    def drain(i, sem):
        some = hub_bufs[i].at[pl.ds(0, n - 1)]
        pltpu.make_async_copy(some, some, sem.at[i]).wait()

    for hop in range(HOPS):
        for c in range(chunks):
            i = hop * chunks + c
            j = i + chunks
            drain(i, hub_recv_sem)

            @pl.when(me > 0)
            def _():
                rim_copy(i, 1).wait_recv()

            @pl.when(me < n - 1)
            def _():
                rim_copy(i, 0).wait_recv()

            hubs = hub_bufs[i][...].reshape(n * hub_dev, LANES)

            def one(b, carry):
                rows = pl.ds(pl.multiple_of(b * tile, tile), tile)
                left = jnp.concatenate([tiles[b, k] for k in range(taps)], axis=1)
                right = jnp.concatenate(
                    [exts[i][cols_ref[b, k]] for k in range(taps)], axis=0
                )
                y = jnp.dot(left, right, preferred_element_type=jnp.float32)
                y = y + jnp.dot(weight[rows, :], hubs, preferred_element_type=jnp.float32)
                x = (y * inv[b]).astype(jnp.bfloat16)
                if c < f_chunks:
                    out_f[hop, rows, c * LANES : (c + 1) * LANES] = x
                else:
                    e = c - f_chunks
                    out_e[hop, rows, e * LANES : (e + 1) * LANES] = x
                if hop + 1 < HOPS:
                    z = (x.astype(jnp.float32) * inv[b]).astype(jnp.bfloat16)
                    locals_[j][b] = z
                    groups[j][pl.ds(b * per, per)] = z.reshape(per, 16, LANES)
                    exts[j][b] = z
                return carry

            lax.fori_loop(0, blocks, one, 0)
            if hop + 1 < HOPS:
                send(j)

    for i in range(pairs):
        drain(i, hub_send_sem)

        @pl.when(me < n - 1)
        def _():
            rim_copy(i, 1).wait_send()

        @pl.when(me > 0)
        def _():
            rim_copy(i, 0).wait_send()


def body(
    features, embeddings, tile_values, tile_columns, send_blocks, send_count,
    hub_rows, hub_weight, degree,
):
    n = lax.axis_size("dom")
    rows = features.shape[0]
    blocks, taps, tile, _ = tile_values.shape
    send_most = send_blocks.shape[2]
    hub_dev = hub_rows.shape[0]
    f_chunks = features.shape[1] // LANES
    chunks = f_chunks + embeddings.shape[1] // LANES
    pairs = HOPS * chunks
    sizes = (blocks, tile, taps, send_most, hub_dev, chunks, f_chunks)
    smem = pl.BlockSpec(memory_space=pltpu.SMEM)
    vmem = pl.BlockSpec(memory_space=pltpu.VMEM)
    bf16 = jnp.bfloat16
    return pl.pallas_call(
        functools.partial(kernel, n, sizes),
        out_shape=(
            jax.ShapeDtypeStruct((HOPS, rows, features.shape[1]), bf16),
            jax.ShapeDtypeStruct((HOPS, rows, embeddings.shape[1]), bf16),
        ),
        in_specs=[smem] * 4 + [vmem] * 5,
        out_specs=(vmem, vmem),
        scratch_shapes=[pltpu.VMEM((blocks, tile, LANES), bf16)] * pairs
        + [pltpu.VMEM((rows // 16, 16, LANES), bf16)] * pairs
        + [pltpu.VMEM((blocks + 2 * send_most, tile, LANES), bf16)] * pairs
        + [pltpu.VMEM((2, send_most, tile, LANES), bf16)] * pairs
        + [pltpu.VMEM((hub_dev, LANES), bf16)] * pairs
        + [pltpu.VMEM((n, hub_dev, LANES), bf16)] * pairs
        + [
            pltpu.VMEM((blocks, tile, LANES), jnp.float32),
            pltpu.SemaphoreType.DMA((pairs, 2)),
            pltpu.SemaphoreType.DMA((pairs, 2)),
            pltpu.SemaphoreType.DMA((pairs,)),
            pltpu.SemaphoreType.DMA((pairs,)),
        ],
        compiler_params=pltpu.CompilerParams(collective_id=0, has_side_effects=True),
    )(
        tile_columns, send_blocks, send_count, hub_rows,
        features, embeddings, tile_values, hub_weight,
        degree.reshape(blocks, tile),
    )


def solution(mesh):
    placed = (
        P("dom", None),
        P("dom", None),
        P("dom", None, None, None),
        P("dom", None),
        P("dom", None, None),
        P("dom", None),
        P("dom"),
        P("dom", None),
        P("dom"),
    )
    return jax.shard_map(
        body,
        mesh=mesh,
        in_specs=placed,
        out_specs=(P(None, "dom", None), P(None, "dom", None)),
        check_vma=False,
    )
```

```python
import functools

import jax
import jax.numpy as jnp
from jax import lax
from jax.experimental import pallas as pl
from jax.experimental.pallas import tpu as pltpu
from jax.sharding import PartitionSpec as P

HOPS = 3
LANES = 128
VMEM = 67043328
MESH = pl.DeviceIdType.MESH


def kernel(
    n, sizes, cols_ref, listed_ref, count_ref, hubs_ref,
    features_hbm, embeddings_hbm, tiles_hbm, weight_hbm, degree_hbm,
    out_f, out_e, *scratch,
):
    blocks, tile, taps, send_most, hub_dev, chunks, f_chunks = sizes
    per = tile // 16
    pairs = HOPS * chunks
    scratch = list(scratch)
    take = lambda count: [scratch.pop(0) for _ in range(count)]
    locals_, groups, exts, sends, hub_sends, hub_bufs = (take(pairs) for _ in range(6))
    features, embeddings, tiles, weight_t, degree, weight, inv, load_sem, rim_send_sem, rim_recv_sem, hub_send_sem, hub_recv_sem = scratch
    me = lax.axis_index("dom")

    loads = [
        pltpu.make_async_copy(source, held, load_sem.at[q])
        for q, (source, held) in enumerate(
            (
                (degree_hbm, degree),
                (features_hbm, features),
                (embeddings_hbm, embeddings),
                (tiles_hbm, tiles),
                (weight_hbm, weight_t),
            )
        )
    ]
    for load in loads:
        load.start()

    barrier = pltpu.get_barrier_semaphore()

    def greet(step, carry):
        pl.semaphore_signal(
            barrier, inc=1, device_id=(lax.rem(me + step, n),), device_id_type=MESH
        )
        return carry

    lax.fori_loop(1, n, greet, 0)

    loads[0].wait()
    roots = lax.rsqrt(degree[...].astype(jnp.float32)).T
    for b in range(blocks):
        inv[b] = jnp.broadcast_to(roots[:, b : b + 1], (tile, LANES))

    rim_zero = jnp.zeros((send_most, tile, LANES), jnp.bfloat16)

    @pl.when(me == 0)
    def _():
        for i in range(pairs):
            exts[i][blocks : blocks + send_most] = rim_zero

    @pl.when(me == n - 1)
    def _():
        for i in range(pairs):
            exts[i][blocks + send_most :] = rim_zero

    def rim_copy(i, side):
        first = blocks if side == 1 else blocks + send_most
        to = me + 1 if side == 1 else me - 1
        return pltpu.make_async_remote_copy(
            src_ref=sends[i].at[side],
            dst_ref=exts[i].at[pl.ds(first, send_most)],
            send_sem=rim_send_sem.at[i, side],
            recv_sem=rim_recv_sem.at[i, side],
            device_id=(to,),
            device_id_type=MESH,
        )

    def send(i):
        source = locals_[i]
        picked = []
        for q in range(hub_dev):
            row = hubs_ref[q]
            near = groups[i][lax.div(row, 16)].astype(jnp.float32)
            here = lax.broadcasted_iota(jnp.int32, near.shape, 0) == lax.rem(row, 16)
            picked.append(jnp.sum(jnp.where(here, near, 0.0), axis=0, keepdims=True))
        packed = jnp.concatenate(picked, axis=0).astype(jnp.bfloat16)
        hub_sends[i][...] = packed
        hub_bufs[i][me] = packed

        def spread(step, carry):
            pltpu.make_async_remote_copy(
                src_ref=hub_sends[i],
                dst_ref=hub_bufs[i].at[me],
                send_sem=hub_send_sem.at[i],
                recv_sem=hub_recv_sem.at[i],
                device_id=(lax.rem(me + step, n),),
                device_id_type=MESH,
            ).start()
            return carry

        lax.fori_loop(1, n, spread, 0)
        for side in range(2):
            for s in range(send_most):
                block = source[listed_ref[0, side, s]]
                keep = jnp.where(s < count_ref[0, side], 1.0, 0.0).astype(jnp.float32)
                sends[i][side, s] = (block.astype(jnp.float32) * keep).astype(jnp.bfloat16)

        @pl.when(me < n - 1)
        def _():
            rim_copy(i, 1).start()

        @pl.when(me > 0)
        def _():
            rim_copy(i, 0).start()

    def prepare(c):
        def one(b, carry):
            rows = pl.ds(pl.multiple_of(b * tile, tile), tile)
            if c < f_chunks:
                x = features[rows, c * LANES : (c + 1) * LANES]
            else:
                x = embeddings[rows, (c - f_chunks) * LANES : (c - f_chunks + 1) * LANES]
            z = (x.astype(jnp.float32) * inv[b]).astype(jnp.bfloat16)
            locals_[c][b] = z
            groups[c][pl.ds(b * per, per)] = z.reshape(per, 16, LANES)
            exts[c][b] = z
            return carry

        lax.fori_loop(0, blocks, one, 0)

    loads[1].wait()
    loads[2].wait()
    prepare(0)
    pl.semaphore_wait(barrier, n - 1)
    send(0)
    for c in range(1, chunks):
        prepare(c)
        send(c)

    loads[3].wait()
    loads[4].wait()
    weight[...] = weight_t[...].T

    def drain(i, sem):
        some = hub_bufs[i].at[pl.ds(0, n - 1)]
        pltpu.make_async_copy(some, some, sem.at[i]).wait()

    for hop in range(HOPS):
        for c in range(chunks):
            i = hop * chunks + c
            j = i + chunks
            drain(i, hub_recv_sem)

            @pl.when(me > 0)
            def _():
                rim_copy(i, 1).wait_recv()

            @pl.when(me < n - 1)
            def _():
                rim_copy(i, 0).wait_recv()

            hubs = hub_bufs[i][...].reshape(n * hub_dev, LANES)

            def one(b, carry):
                rows = pl.ds(pl.multiple_of(b * tile, tile), tile)
                left = jnp.concatenate([tiles[b, k] for k in range(taps)], axis=1)
                right = jnp.concatenate(
                    [exts[i][cols_ref[k, b]] for k in range(taps)], axis=0
                )
                y = jnp.dot(left, right, preferred_element_type=jnp.float32)
                y = y + jnp.dot(weight[rows, :], hubs, preferred_element_type=jnp.float32)
                x = (y * inv[b]).astype(jnp.bfloat16)
                if c < f_chunks:
                    out_f[hop, rows, c * LANES : (c + 1) * LANES] = x
                else:
                    e = c - f_chunks
                    out_e[hop, rows, e * LANES : (e + 1) * LANES] = x
                if hop + 1 < HOPS:
                    z = (x.astype(jnp.float32) * inv[b]).astype(jnp.bfloat16)
                    locals_[j][b] = z
                    groups[j][pl.ds(b * per, per)] = z.reshape(per, 16, LANES)
                    exts[j][b] = z
                return carry

            lax.fori_loop(0, blocks, one, 0)
            if hop + 1 < HOPS:
                send(j)

    for i in range(pairs):
        drain(i, hub_send_sem)

        @pl.when(me < n - 1)
        def _():
            rim_copy(i, 1).wait_send()

        @pl.when(me > 0)
        def _():
            rim_copy(i, 0).wait_send()


def body(
    features, embeddings, tile_values, tile_columns, send_blocks, send_count,
    hub_rows, hub_weight, degree,
):
    n = lax.axis_size("dom")
    rows = features.shape[0]
    blocks, taps, tile, _ = tile_values.shape
    send_most = send_blocks.shape[2]
    hub_dev = hub_rows.shape[0]
    f_chunks = features.shape[1] // LANES
    chunks = f_chunks + embeddings.shape[1] // LANES
    pairs = HOPS * chunks
    sizes = (blocks, tile, taps, send_most, hub_dev, chunks, f_chunks)
    out_bytes = HOPS * rows * chunks * LANES * 2
    smem = pl.BlockSpec(memory_space=pltpu.SMEM)
    vmem = pl.BlockSpec(memory_space=pltpu.VMEM)
    bf16 = jnp.bfloat16
    return pl.pallas_call(
        functools.partial(kernel, n, sizes),
        out_shape=(
            pltpu.VMEM((HOPS, rows, features.shape[1]), bf16),
            pltpu.VMEM((HOPS, rows, embeddings.shape[1]), bf16),
        ),
        in_specs=[smem] * 4 + [pl.BlockSpec(memory_space=pltpu.HBM)] * 5,
        out_specs=(vmem, vmem),
        scratch_shapes=[pltpu.VMEM((blocks, tile, LANES), bf16)] * pairs
        + [pltpu.VMEM((rows // 16, 16, LANES), bf16)] * pairs
        + [pltpu.VMEM((blocks + 2 * send_most, tile, LANES), bf16)] * pairs
        + [pltpu.VMEM((2, send_most, tile, LANES), bf16)] * pairs
        + [pltpu.VMEM((hub_dev, LANES), bf16)] * pairs
        + [pltpu.VMEM((n, hub_dev, LANES), bf16)] * pairs
        + [
            pltpu.VMEM(features.shape, bf16),
            pltpu.VMEM(embeddings.shape, bf16),
            pltpu.VMEM(tile_values.shape, bf16),
            pltpu.VMEM((n * hub_dev, rows), bf16),
            pltpu.VMEM((blocks, tile), jnp.int32),
            pltpu.VMEM((rows, n * hub_dev), bf16),
            pltpu.VMEM((blocks, tile, LANES), jnp.float32),
            pltpu.SemaphoreType.DMA((5,)),
            pltpu.SemaphoreType.DMA((pairs, 2)),
            pltpu.SemaphoreType.DMA((pairs, 2)),
            pltpu.SemaphoreType.DMA((pairs,)),
            pltpu.SemaphoreType.DMA((pairs,)),
        ],
        compiler_params=pltpu.CompilerParams(
            collective_id=0, has_side_effects=True, vmem_limit_bytes=VMEM - out_bytes
        ),
    )(
        tile_columns.T, send_blocks, send_count, hub_rows,
        features, embeddings, tile_values, hub_weight.T,
        degree.reshape(blocks, tile),
    )


def solution(mesh):
    placed = (
        P("dom", None),
        P("dom", None),
        P("dom", None, None, None),
        P("dom", None),
        P("dom", None, None),
        P("dom", None),
        P("dom"),
        P("dom", None),
        P("dom"),
    )
    return jax.shard_map(
        body,
        mesh=mesh,
        in_specs=placed,
        out_specs=(P(None, "dom", None), P(None, "dom", None)),
        check_vma=False,
    )
```

```python
import functools

import jax
import jax.numpy as jnp
from jax import lax
from jax.experimental import pallas as pl
from jax.experimental.pallas import tpu as pltpu
from jax.sharding import PartitionSpec as P

HOPS = 3
LANES = 128
WIDTH = 256
UNROLL = 4
VMEM = 67043328
MESH = pl.DeviceIdType.MESH


def cut(which, columns):
    return [(which, at, min(WIDTH, columns - at)) for at in range(0, columns, WIDTH)]


def kernel(
    n, sizes, cols_ref, listed_ref, count_ref, hubs_ref,
    features_hbm, embeddings_hbm, tiles_hbm, weight_hbm, degree_hbm,
    out_f, out_e, *scratch,
):
    blocks, tile, taps, send_most, hub_dev, pieces = sizes
    chunks = len(pieces)
    per = tile // 16
    pairs = HOPS * chunks
    scratch = list(scratch)
    take = lambda count: [scratch.pop(0) for _ in range(count)]
    locals_, groups, exts, sends, hub_sends, hub_bufs = (take(pairs) for _ in range(6))
    features, embeddings, tiles, weight_t, degree, weight, inv, load_sem, rim_send_sem, rim_recv_sem, hub_send_sem, hub_recv_sem = scratch
    me = lax.axis_index("dom")

    loads = [
        pltpu.make_async_copy(source, held, load_sem.at[q])
        for q, (source, held) in enumerate(
            (
                (degree_hbm, degree),
                (features_hbm, features),
                (embeddings_hbm, embeddings),
                (tiles_hbm, tiles),
                (weight_hbm, weight_t),
            )
        )
    ]
    for load in loads:
        load.start()

    barrier = pltpu.get_barrier_semaphore()

    def greet(step, carry):
        pl.semaphore_signal(
            barrier, inc=1, device_id=(lax.rem(me + step, n),), device_id_type=MESH
        )
        return carry

    lax.fori_loop(1, n, greet, 0)

    loads[0].wait()
    roots = lax.rsqrt(degree[...].astype(jnp.float32)).T
    for b in range(blocks):
        inv[b] = jnp.broadcast_to(roots[:, b : b + 1], (tile, LANES))

    def wide(b, width):
        return jnp.concatenate([inv[b]] * (width // LANES), axis=1)

    @pl.when(me == 0)
    def _():
        for i in range(pairs):
            exts[i][blocks : blocks + send_most] = jnp.zeros((send_most,) + exts[i].shape[1:], jnp.bfloat16)

    @pl.when(me == n - 1)
    def _():
        for i in range(pairs):
            exts[i][blocks + send_most :] = jnp.zeros((send_most,) + exts[i].shape[1:], jnp.bfloat16)

    def rim_copy(i, side):
        first = blocks if side == 1 else blocks + send_most
        to = me + 1 if side == 1 else me - 1
        return pltpu.make_async_remote_copy(
            src_ref=sends[i].at[side],
            dst_ref=exts[i].at[pl.ds(first, send_most)],
            send_sem=rim_send_sem.at[i, side],
            recv_sem=rim_recv_sem.at[i, side],
            device_id=(to,),
            device_id_type=MESH,
        )

    def send(i):
        source = locals_[i]
        picked = []
        for q in range(hub_dev):
            row = hubs_ref[q]
            near = groups[i][lax.div(row, 16)].astype(jnp.float32)
            here = lax.broadcasted_iota(jnp.int32, near.shape, 0) == lax.rem(row, 16)
            picked.append(jnp.sum(jnp.where(here, near, 0.0), axis=0, keepdims=True))
        packed = jnp.concatenate(picked, axis=0).astype(jnp.bfloat16)
        hub_sends[i][...] = packed
        hub_bufs[i][me] = packed

        def spread(step, carry):
            pltpu.make_async_remote_copy(
                src_ref=hub_sends[i],
                dst_ref=hub_bufs[i].at[me],
                send_sem=hub_send_sem.at[i],
                recv_sem=hub_recv_sem.at[i],
                device_id=(lax.rem(me + step, n),),
                device_id_type=MESH,
            ).start()
            return carry

        lax.fori_loop(1, n, spread, 0)
        for side in range(2):
            for s in range(send_most):
                block = source[listed_ref[0, side, s]]
                keep = jnp.where(s < count_ref[0, side], 1.0, 0.0).astype(jnp.float32)
                sends[i][side, s] = (block.astype(jnp.float32) * keep).astype(jnp.bfloat16)

        @pl.when(me < n - 1)
        def _():
            rim_copy(i, 1).start()

        @pl.when(me > 0)
        def _():
            rim_copy(i, 0).start()

    def prepare(c):
        which, at, width = pieces[c]

        def one(b, carry):
            rows = pl.ds(pl.multiple_of(b * tile, tile), tile)
            x = (features, embeddings)[which][rows, at : at + width]
            z = (x.astype(jnp.float32) * wide(b, width)).astype(jnp.bfloat16)
            locals_[c][b] = z
            groups[c][pl.ds(b * per, per)] = z.reshape(per, 16, width)
            exts[c][b] = z
            return carry

        lax.fori_loop(0, blocks, one, 0, unroll=UNROLL)

    loads[1].wait()
    loads[2].wait()
    prepare(0)
    pl.semaphore_wait(barrier, n - 1)
    send(0)
    for c in range(1, chunks):
        prepare(c)
        send(c)

    loads[3].wait()
    loads[4].wait()
    weight[...] = weight_t[...].T

    def drain(i, sem):
        some = hub_bufs[i].at[pl.ds(0, n - 1)]
        pltpu.make_async_copy(some, some, sem.at[i]).wait()

    for hop in range(HOPS):
        for c in range(chunks):
            i = hop * chunks + c
            j = i + chunks
            which, at, width = pieces[c]
            drain(i, hub_recv_sem)

            @pl.when(me > 0)
            def _():
                rim_copy(i, 1).wait_recv()

            @pl.when(me < n - 1)
            def _():
                rim_copy(i, 0).wait_recv()

            hubs = hub_bufs[i][...].reshape(n * hub_dev, width)

            def one(b, carry):
                rows = pl.ds(pl.multiple_of(b * tile, tile), tile)
                left = jnp.concatenate([tiles[b, k] for k in range(taps)], axis=1)
                right = jnp.concatenate(
                    [exts[i][cols_ref[k, b]] for k in range(taps)], axis=0
                )
                y = jnp.dot(left, right, preferred_element_type=jnp.float32)
                y = y + jnp.dot(weight[rows, :], hubs, preferred_element_type=jnp.float32)
                root = wide(b, width)
                x = (y * root).astype(jnp.bfloat16)
                (out_f, out_e)[which][hop, rows, at : at + width] = x
                if hop + 1 < HOPS:
                    z = (x.astype(jnp.float32) * root).astype(jnp.bfloat16)
                    locals_[j][b] = z
                    groups[j][pl.ds(b * per, per)] = z.reshape(per, 16, width)
                    exts[j][b] = z
                return carry

            lax.fori_loop(0, blocks, one, 0, unroll=UNROLL)
            if hop + 1 < HOPS:
                send(j)

    for i in range(pairs):
        drain(i, hub_send_sem)

        @pl.when(me < n - 1)
        def _():
            rim_copy(i, 1).wait_send()

        @pl.when(me > 0)
        def _():
            rim_copy(i, 0).wait_send()


def body(
    features, embeddings, tile_values, tile_columns, send_blocks, send_count,
    hub_rows, hub_weight, degree,
):
    n = lax.axis_size("dom")
    rows = features.shape[0]
    blocks, taps, tile, _ = tile_values.shape
    send_most = send_blocks.shape[2]
    hub_dev = hub_rows.shape[0]
    pieces = cut(0, features.shape[1]) + cut(1, embeddings.shape[1])
    sizes = (blocks, tile, taps, send_most, hub_dev, pieces)
    widths = [width for _, _, width in pieces] * HOPS
    out_bytes = HOPS * rows * (features.shape[1] + embeddings.shape[1]) * 2
    smem = pl.BlockSpec(memory_space=pltpu.SMEM)
    vmem = pl.BlockSpec(memory_space=pltpu.VMEM)
    bf16 = jnp.bfloat16
    return pl.pallas_call(
        functools.partial(kernel, n, sizes),
        out_shape=(
            pltpu.VMEM((HOPS, rows, features.shape[1]), bf16),
            pltpu.VMEM((HOPS, rows, embeddings.shape[1]), bf16),
        ),
        in_specs=[smem] * 4 + [pl.BlockSpec(memory_space=pltpu.HBM)] * 5,
        out_specs=(vmem, vmem),
        scratch_shapes=[
            pltpu.VMEM(shape + (width,), bf16)
            for shape in (
                (blocks, tile),
                (rows // 16, 16),
                (blocks + 2 * send_most, tile),
                (2, send_most, tile),
                (hub_dev,),
                (n, hub_dev),
            )
            for width in widths
        ]
        + [
            pltpu.VMEM(features.shape, bf16),
            pltpu.VMEM(embeddings.shape, bf16),
            pltpu.VMEM(tile_values.shape, bf16),
            pltpu.VMEM((n * hub_dev, rows), bf16),
            pltpu.VMEM((blocks, tile), jnp.int32),
            pltpu.VMEM((rows, n * hub_dev), bf16),
            pltpu.VMEM((blocks, tile, LANES), jnp.float32),
            pltpu.SemaphoreType.DMA((5,)),
            pltpu.SemaphoreType.DMA((len(widths), 2)),
            pltpu.SemaphoreType.DMA((len(widths), 2)),
            pltpu.SemaphoreType.DMA((len(widths),)),
            pltpu.SemaphoreType.DMA((len(widths),)),
        ],
        compiler_params=pltpu.CompilerParams(
            collective_id=0, has_side_effects=True, vmem_limit_bytes=VMEM - out_bytes
        ),
    )(
        tile_columns.T, send_blocks, send_count, hub_rows,
        features, embeddings, tile_values, hub_weight.T,
        degree.reshape(blocks, tile),
    )


def solution(mesh):
    placed = (
        P("dom", None),
        P("dom", None),
        P("dom", None, None, None),
        P("dom", None),
        P("dom", None, None),
        P("dom", None),
        P("dom"),
        P("dom", None),
        P("dom"),
    )
    return jax.shard_map(
        body,
        mesh=mesh,
        in_specs=placed,
        out_specs=(P(None, "dom", None), P(None, "dom", None)),
        check_vma=False,
    )
```

```python
import functools

import jax
import jax.numpy as jnp
from jax import lax
from jax.experimental import pallas as pl
from jax.experimental.pallas import tpu as pltpu
from jax.sharding import PartitionSpec as P

HOPS = 3
LANES = 128
WIDTH = 256
UNROLL = 4
VMEM = 67043328
MESH = pl.DeviceIdType.MESH


def cut(which, columns):
    return [(which, at, min(WIDTH, columns - at)) for at in range(0, columns, WIDTH)]


def kernel(
    n, sizes, cols_ref, listed_ref, count_ref, hubs_ref,
    features_hbm, embeddings_hbm, tiles_hbm, weight_hbm, degree_hbm,
    out_f, out_e, *scratch,
):
    blocks, tile, taps, send_most, hub_dev, pieces = sizes
    chunks = len(pieces)
    per = tile // 16
    pairs = HOPS * chunks
    scratch = list(scratch)
    take = lambda count: [scratch.pop(0) for _ in range(count)]
    locals_, groups, exts, sends, hub_sends, hub_bufs = (take(pairs) for _ in range(6))
    features, embeddings, tiles, weight_t, degree, weight, inv, load_sem, rim_send_sem, rim_recv_sem, hub_send_sem, hub_recv_sem = scratch
    me = lax.axis_index("dom")

    loads = [
        pltpu.make_async_copy(source, held, load_sem.at[q])
        for q, (source, held) in enumerate(
            (
                (degree_hbm, degree),
                (features_hbm, features),
                (embeddings_hbm, embeddings),
                (tiles_hbm, tiles),
                (weight_hbm, weight_t),
            )
        )
    ]
    for load in loads:
        load.start()

    barrier = pltpu.get_barrier_semaphore()

    def greet(step, carry):
        pl.semaphore_signal(
            barrier, inc=1, device_id=(lax.rem(me + step, n),), device_id_type=MESH
        )
        return carry

    lax.fori_loop(1, n, greet, 0)

    loads[0].wait()
    roots = lax.rsqrt(degree[...].astype(jnp.float32)).T
    for b in range(blocks):
        inv[b] = jnp.broadcast_to(roots[:, b : b + 1], (tile, LANES))

    def wide(b, width):
        return jnp.concatenate([inv[b]] * (width // LANES), axis=1)

    @pl.when(me == 0)
    def _():
        for i in range(pairs):
            exts[i][blocks : blocks + send_most] = jnp.zeros((send_most,) + exts[i].shape[1:], jnp.bfloat16)

    @pl.when(me == n - 1)
    def _():
        for i in range(pairs):
            exts[i][blocks + send_most :] = jnp.zeros((send_most,) + exts[i].shape[1:], jnp.bfloat16)

    def rim_copy(i, side):
        first = blocks if side == 1 else blocks + send_most
        to = me + 1 if side == 1 else me - 1
        return pltpu.make_async_remote_copy(
            src_ref=sends[i].at[side],
            dst_ref=exts[i].at[pl.ds(first, send_most)],
            send_sem=rim_send_sem.at[i, side],
            recv_sem=rim_recv_sem.at[i, side],
            device_id=(to,),
            device_id_type=MESH,
        )

    def stage(i):
        source = locals_[i]
        picked = []
        for q in range(hub_dev):
            row = hubs_ref[q]
            near = groups[i][lax.div(row, 16)].astype(jnp.float32)
            here = lax.broadcasted_iota(jnp.int32, near.shape, 0) == lax.rem(row, 16)
            picked.append(jnp.sum(jnp.where(here, near, 0.0), axis=0, keepdims=True))
        packed = jnp.concatenate(picked, axis=0).astype(jnp.bfloat16)
        hub_sends[i][...] = packed
        hub_bufs[i][me] = packed

        for side in range(2):
            for s in range(send_most):
                block = source[listed_ref[0, side, s]]
                keep = jnp.where(s < count_ref[0, side], 1.0, 0.0).astype(jnp.float32)
                sends[i][side, s] = (block.astype(jnp.float32) * keep).astype(jnp.bfloat16)


    def launch(i):
        def spread(step, carry):
            pltpu.make_async_remote_copy(
                src_ref=hub_sends[i],
                dst_ref=hub_bufs[i].at[me],
                send_sem=hub_send_sem.at[i],
                recv_sem=hub_recv_sem.at[i],
                device_id=(lax.rem(me + step, n),),
                device_id_type=MESH,
            ).start()
            return carry

        lax.fori_loop(1, n, spread, 0)

        @pl.when(me < n - 1)
        def _():
            rim_copy(i, 1).start()

        @pl.when(me > 0)
        def _():
            rim_copy(i, 0).start()

    def prepare(c):
        which, at, width = pieces[c]

        def one(b, carry):
            rows = pl.ds(pl.multiple_of(b * tile, tile), tile)
            x = (features, embeddings)[which][rows, at : at + width]
            z = (x.astype(jnp.float32) * wide(b, width)).astype(jnp.bfloat16)
            locals_[c][b] = z
            groups[c][pl.ds(b * per, per)] = z.reshape(per, 16, width)
            exts[c][b] = z
            return carry

        lax.fori_loop(0, blocks, one, 0, unroll=UNROLL)

    loads[1].wait()
    loads[2].wait()
    for c in range(chunks):
        prepare(c)
        stage(c)
    pl.semaphore_wait(barrier, n - 1)
    for c in range(chunks):
        launch(c)

    loads[3].wait()
    loads[4].wait()
    weight[...] = weight_t[...].T

    def drain(i, sem):
        some = hub_bufs[i].at[pl.ds(0, n - 1)]
        pltpu.make_async_copy(some, some, sem.at[i]).wait()

    for hop in range(HOPS):
        for c in range(chunks):
            i = hop * chunks + c
            j = i + chunks
            which, at, width = pieces[c]
            drain(i, hub_recv_sem)

            @pl.when(me > 0)
            def _():
                rim_copy(i, 1).wait_recv()

            @pl.when(me < n - 1)
            def _():
                rim_copy(i, 0).wait_recv()

            hubs = hub_bufs[i][...].reshape(n * hub_dev, width)

            def one(b, carry):
                rows = pl.ds(pl.multiple_of(b * tile, tile), tile)
                left = jnp.concatenate([tiles[b, k] for k in range(taps)], axis=1)
                right = jnp.concatenate(
                    [exts[i][cols_ref[k, b]] for k in range(taps)], axis=0
                )
                y = jnp.dot(left, right, preferred_element_type=jnp.float32)
                y = y + jnp.dot(weight[rows, :], hubs, preferred_element_type=jnp.float32)
                root = wide(b, width)
                x = (y * root).astype(jnp.bfloat16)
                (out_f, out_e)[which][hop, rows, at : at + width] = x
                if hop + 1 < HOPS:
                    z = (x.astype(jnp.float32) * root).astype(jnp.bfloat16)
                    locals_[j][b] = z
                    groups[j][pl.ds(b * per, per)] = z.reshape(per, 16, width)
                    exts[j][b] = z
                return carry

            lax.fori_loop(0, blocks, one, 0, unroll=UNROLL)
            if hop + 1 < HOPS:
                stage(j)
                launch(j)

    for i in range(pairs):
        drain(i, hub_send_sem)

        @pl.when(me < n - 1)
        def _():
            rim_copy(i, 1).wait_send()

        @pl.when(me > 0)
        def _():
            rim_copy(i, 0).wait_send()


def flush(held_f, held_e, out_f, out_e, sem):
    copies = [
        pltpu.make_async_copy(held_f, out_f, sem.at[0]),
        pltpu.make_async_copy(held_e, out_e, sem.at[1]),
    ]
    for copy in copies:
        copy.start()
    for copy in copies:
        copy.wait()


def body(
    features, embeddings, tile_values, tile_columns, send_blocks, send_count,
    hub_rows, hub_weight, degree,
):
    n = lax.axis_size("dom")
    rows = features.shape[0]
    blocks, taps, tile, _ = tile_values.shape
    send_most = send_blocks.shape[2]
    hub_dev = hub_rows.shape[0]
    pieces = cut(0, features.shape[1]) + cut(1, embeddings.shape[1])
    sizes = (blocks, tile, taps, send_most, hub_dev, pieces)
    widths = [width for _, _, width in pieces] * HOPS
    out_bytes = HOPS * rows * (features.shape[1] + embeddings.shape[1]) * 2
    smem = pl.BlockSpec(memory_space=pltpu.SMEM)
    vmem = pl.BlockSpec(memory_space=pltpu.VMEM)
    bf16 = jnp.bfloat16
    held = pl.pallas_call(
        functools.partial(kernel, n, sizes),
        out_shape=(
            pltpu.VMEM((HOPS, rows, features.shape[1]), bf16),
            pltpu.VMEM((HOPS, rows, embeddings.shape[1]), bf16),
        ),
        in_specs=[smem] * 4 + [pl.BlockSpec(memory_space=pltpu.HBM)] * 5,
        out_specs=(vmem, vmem),
        scratch_shapes=[
            pltpu.VMEM(shape + (width,), bf16)
            for shape in (
                (blocks, tile),
                (rows // 16, 16),
                (blocks + 2 * send_most, tile),
                (2, send_most, tile),
                (hub_dev,),
                (n, hub_dev),
            )
            for width in widths
        ]
        + [
            pltpu.VMEM(features.shape, bf16),
            pltpu.VMEM(embeddings.shape, bf16),
            pltpu.VMEM(tile_values.shape, bf16),
            pltpu.VMEM((n * hub_dev, rows), bf16),
            pltpu.VMEM((blocks, tile), jnp.int32),
            pltpu.VMEM((rows, n * hub_dev), bf16),
            pltpu.VMEM((blocks, tile, LANES), jnp.float32),
            pltpu.SemaphoreType.DMA((5,)),
            pltpu.SemaphoreType.DMA((len(widths), 2)),
            pltpu.SemaphoreType.DMA((len(widths), 2)),
            pltpu.SemaphoreType.DMA((len(widths),)),
            pltpu.SemaphoreType.DMA((len(widths),)),
        ],
        compiler_params=pltpu.CompilerParams(
            collective_id=0, has_side_effects=True, vmem_limit_bytes=VMEM - out_bytes
        ),
    )(
        tile_columns.T, send_blocks, send_count, hub_rows,
        features, embeddings, tile_values, hub_weight.T,
        degree.reshape(blocks, tile),
    )
    hbm = pl.BlockSpec(memory_space=pltpu.HBM)
    return pl.pallas_call(
        flush,
        out_shape=tuple(jax.ShapeDtypeStruct(h.shape, h.dtype) for h in held),
        in_specs=[vmem] * 2,
        out_specs=(hbm, hbm),
        scratch_shapes=[pltpu.SemaphoreType.DMA((2,))],
        compiler_params=pltpu.CompilerParams(vmem_limit_bytes=2**20),
    )(*held)


def solution(mesh):
    placed = (
        P("dom", None),
        P("dom", None),
        P("dom", None, None, None),
        P("dom", None),
        P("dom", None, None),
        P("dom", None),
        P("dom"),
        P("dom", None),
        P("dom"),
    )
    return jax.shard_map(
        body,
        mesh=mesh,
        in_specs=placed,
        out_specs=(P(None, "dom", None), P(None, "dom", None)),
        check_vma=False,
    )
```
